256 devices in a mesh: groups: 2 (over z), owners: 16 (over x, core), sub: 8 (over y).
Axes of the slice: x: 8, y: 8, z: 2, core: 2. Of those that a mesh axis runs over, the one named last changes fastest.
The devices are a block of a 8x8x16 slice.
Arguments:
- embeddings: bfloat16 [131072, 768], P(('groups', 'owners', 'sub')), parts along dimension 0, may hold values from -6 to 6, as said below
- class_table: bfloat16 [1000, 768], replicated, may hold values from -6 to 6
- nearest: int32 [131072], P(('groups', 'owners', 'sub')), parts along dimension 0, may hold values from 0 to 999
- keep_class: int32 [1000], replicated, may hold values 0 or 1
- destination: int32 [131072, 1], P(('groups', 'owners', 'sub')), parts along dimension 0, may hold values from 0 to 127; in each aligned block of 512 rows (0 to 511, 512 to 1023, ...) at most 6 rows name the same one
Outputs:
- received_rows: bfloat16 [196608, 768], P(('groups', 'owners', 'sub')), parts along dimension 0
- received_score: bfloat16 [196608], P(('groups', 'owners', 'sub')), parts along dimension 0
- received_position: int32 [196608], P(('groups', 'owners', 'sub')), parts along dimension 0
- shard_totals: int32 [256], P('groups'), parts along dimension 0
The draws below stay inside these ranges and needn't reach their ends.
There are 2 independent parts, one for each index of `groups`. The reference program is written for one: setup_inputs(seed, part) draws one part's arguments, and reference() takes and returns one part's arrays. A program takes and returns all parts, laid end to end along the dimension named above; an argument that names none is the same for every part. Nothing has to cross between parts.
Inputs may be any that keep to these rules, and one draw needn't show every extreme that they name: `destination`: in the rows of one device no loader shard is named by more than 6 rows. Counts of rows per loader shard may be packed several to an int32 word wherever they travel; this is an exception to the 16-bit rule below. `embeddings`: some rows are entirely zero.
All inputs are finite; a program needn't handle non-finite values.
Results may differ from the reference program's by a relative error of at most 0.001.
Values may be sent and summed in bfloat16 or wider, within the bound.
No kernel may reach another device: no remote copies, remote signals or barrier semaphores. Data moves between devices by JAX's collectives and lax.ppermute only.
A program may use at most 64 MiB of HBM per device.

```python
import math
import jax
import jax.numpy as jnp
import numpy as np
from jax import lax

D = 768
CLASSES = 1000
ROWS_DEV = 512
NDEST = 128
CAP = 6
ROWS = 65536


def draw_embeddings(key, part):
    value_key = jax.random.fold_in(key, 11)
    blank_key = jax.random.fold_in(key, 13)
    values = jnp.clip(jax.random.normal(value_key, (ROWS, D), jnp.float32), -6.0, 6.0)
    blank = jax.random.randint(blank_key, (ROWS, 1), 0, 64) == 0
    values = jnp.where(blank, jnp.float32(0.0), values)
    return values.astype(jnp.bfloat16)


def plant(values, own_key, least, high):
    dims = values.shape
    spot = [jax.random.randint(jax.random.fold_in(own_key, axis), (), 0, dims[axis]) for axis in range(len(dims))]
    values = values.at[tuple(spot)].set(least)
    longest = dims.index(max(dims))
    spot[longest] = (spot[longest] + 1) % dims[longest]
    return values.at[tuple(spot)].set(high)


def routed_block(rng, own, number, rows, count, top, bound, slope):
    ranking = jax.random.permutation(rng, count)
    heavy_load, ordinary = shares(count, rows * top, bound, slope, True), shares(count, rows * top, bound, slope, False)
    places = jnp.arange(count)

    def named(tallies, turn):
        used = int((tallies > 0).sum())
        fixed = max(1, used // 4)
        passed = fixed + (places - fixed + turn * (used - fixed)) % max(1, count - fixed)
        return jnp.zeros((count,), jnp.int32).at[ranking[jnp.where(places < fixed, places, passed)]].set(jnp.asarray(tallies, jnp.int32))

    tallies = jnp.where(number % 4 == 0, named(heavy_load, number // 4), named(ordinary, number - number // 4 - 1))
    mixed = jax.random.permutation(jax.random.fold_in(own, 3), count)
    donor, taker = mixed[0:count // 2 * 2:2], mixed[1:count // 2 * 2:2]
    slack = jnp.minimum(tallies[donor] - 1, bound - tallies[taker]) // 2
    slack = jnp.where((donor == ranking[0]) | (taker == ranking[0]) | (tallies[taker] == 0), 0, jnp.maximum(slack, 0))
    passed = jax.random.randint(jax.random.fold_in(own, 4), (count // 2,), 0, 1 << 20) % (slack + 1)
    tallies = tallies.at[donor].add(-passed).at[taker].add(passed)
    items = jnp.searchsorted(jnp.cumsum(tallies), jnp.arange(rows * top), side="right").astype(jnp.int32)
    table = items.reshape(top, rows).T
    table = table[jax.random.permutation(jax.random.fold_in(own, 1), rows)]
    turn = jax.random.randint(jax.random.fold_in(own, 2), (rows, 1), 0, top)
    return jnp.take_along_axis(table, (jnp.arange(top)[None, :] + turn) % top, axis=1)


def shares(amount, total, bound, lean, full):
    portions = [(1 << 20) // math.isqrt(rank ** lean) + 1 for rank in range(1, amount + 1)]
    largest = bound if full else min(bound, max(-(-total // amount), total * portions[0] // sum(portions)))
    least = 1 if total - largest >= amount - 1 else 0
    holding, rest = [largest] + [least] * (amount - 1), total - largest - least * (amount - 1)
    while rest > 0:
        candidates = [i for i in range(1, amount) if holding[i] < largest] or [i for i in range(1, amount) if holding[i] < bound]
        mass, budget = sum([portions[i] for i in candidates]), rest
        for i in candidates:
            more = min(bound - holding[i], max(1, budget * portions[i] // mass), rest)
            holding[i] = holding[i] + more
            rest = rest - more
    return np.array(holding)


def noise(stream_key, extent, scale, most, kind=jnp.bfloat16):
    return jnp.clip(scale * jax.random.normal(stream_key, extent, jnp.float32), -most, most).astype(kind)


def setup_inputs(seed: int = 0, part: int = 0) -> dict:
    keys = jax.random.split(jax.random.key(seed), 6)
    own_keys = jax.random.split(jax.random.fold_in(keys[5], part), 6)
    embeddings = draw_embeddings(jax.random.fold_in(jax.random.fold_in(keys[5], part), 71), part)
    class_table = noise(keys[1], (CLASSES, D), 1.0, 6.0)
    nearest = plant(jax.random.randint(own_keys[2], (ROWS,), 0, CLASSES), jax.random.fold_in(own_keys[2], 1), 0, CLASSES - 1).astype(jnp.int32)
    keep_class = plant((jax.random.randint(keys[3], (CLASSES,), 0, 4) < 3).astype(jnp.int32), jax.random.fold_in(keys[3], 1), 0, 1)
    destination_keys = jax.random.split(jax.random.fold_in(own_keys[4], 1), ROWS // ROWS_DEV)
    destination_turns = jax.random.permutation(jax.random.fold_in(own_keys[4], 3), ROWS // ROWS_DEV)
    destination = jax.vmap(lambda own, number: routed_block(jax.random.fold_in(own_keys[4], 2), own, number, ROWS_DEV, NDEST, 1, CAP, 2))(destination_keys, destination_turns).reshape((ROWS, 1))
    return dict(embeddings=embeddings, class_table=class_table, nearest=nearest, keep_class=keep_class, destination=destination)


def margins(row_block, near_block, class_table, inverse_class, keep_class):
    products = jnp.dot(row_block, class_table.T, preferred_element_type=jnp.float32)
    squares = row_block.astype(jnp.float32) * row_block.astype(jnp.float32)
    inverse_row = lax.rsqrt(lax.optimization_barrier(jnp.sum(squares, axis=1)) + 1e-06)
    cosine = products * inverse_row[:, None] * inverse_class[None, :]
    class_ids = jnp.arange(class_table.shape[0], dtype=jnp.int32)
    class_match = near_block[:, None] == class_ids[None, :]
    given_cos = lax.optimization_barrier(jnp.sum(jnp.where(class_match, cosine, 0.0), axis=1))
    others = lax.optimization_barrier(jnp.max(jnp.where(class_match, -1e+30, cosine), axis=1))
    kept_flag = lax.optimization_barrier(jnp.sum(jnp.where(class_match, keep_class[None, :], 0), axis=1)).astype(jnp.int32)
    return (20.0 * (given_cos - others), kept_flag)

def reference(embeddings, class_table, nearest, keep_class, destination):
    class_float = class_table.astype(jnp.float32)
    inverse_class = lax.rsqrt(lax.optimization_barrier(jnp.sum(class_float * class_float, axis=1)) + 1e-06)
    total_rows = embeddings.shape[0]
    block_rows = math.gcd(total_rows, 1024)

    def one_block(inputs):
        return margins(inputs[0], inputs[1], class_table, inverse_class, keep_class)
    margin_value, kept_flag = lax.map(one_block, (embeddings.reshape(total_rows // block_rows, block_rows, D), nearest.reshape(total_rows // block_rows, block_rows)))
    margin_value = margin_value.reshape(total_rows)
    kept_flag = kept_flag.reshape(total_rows)
    target = destination[:, 0].astype(jnp.int32)
    shard_ids = jnp.arange(NDEST, dtype=jnp.int32)
    onehot = ((target[:, None] == shard_ids[None, :]) & (kept_flag[:, None] == 1)).astype(jnp.int32)
    running = jnp.cumsum(onehot, axis=0) - onehot
    global_rank = jnp.take_along_axis(running, target[:, None], axis=1)[:, 0].astype(jnp.int32)
    block_start = running.reshape(NDEST, ROWS_DEV, NDEST)[:, 0, :]
    source = (jnp.arange(total_rows, dtype=jnp.int32) // ROWS_DEV).astype(jnp.int32)
    local_rank = (global_rank - block_start[source, target]).astype(jnp.int32)
    slot_count = NDEST * NDEST * CAP
    slot_index = jnp.where(kept_flag == 1, (target * NDEST + source) * CAP + local_rank, slot_count).astype(jnp.int32)
    received_rows = jnp.zeros((slot_count, D), jnp.bfloat16).at[slot_index].set(embeddings, mode='drop')
    received_score = jnp.zeros((slot_count,), jnp.bfloat16).at[slot_index].set(margin_value.astype(jnp.bfloat16), mode='drop')
    received_position = jnp.full((slot_count,), -1, jnp.int32).at[slot_index].set(global_rank, mode='drop')
    shard_totals = lax.optimization_barrier(jnp.sum(onehot, axis=0)).astype(jnp.int32)
    return (received_rows, received_score, received_position, shard_totals)
```

```python
import jax
import jax.numpy as jnp
from jax import lax
from jax.experimental import pallas as pl
from jax.experimental.pallas import tpu as pltpu
from jax.sharding import PartitionSpec as P

GROUP = ("owners", "sub")
ALL = ("groups", "owners", "sub")
LANES = 128
CHUNK = 256
F32 = jnp.float32
BF16 = jnp.bfloat16
NT = (((1,), (1,)), ((), ()))
NN = (((1,), (0,)), ((), ()))


def dot(a, b, dims=NN):
    return lax.dot_general(a, b, dims, preferred_element_type=F32)


def iota(shape, dim):
    return lax.broadcasted_iota(jnp.int32, shape, dim)


def mask(cond):
    return jnp.where(cond, 1.0, 0.0)


def pack_kernel(me, nearest, keep, target, emb_hbm, table_hbm, out, emb, table, sems):
    rows, width = emb.shape
    classes = table.shape[0]
    shards = out.shape[0] // 8
    cap = 3 * rows // (2 * shards)
    head = out.shape[1]
    get_emb = pltpu.make_async_copy(emb_hbm, emb, sems.at[0])
    get_table = pltpu.make_async_copy(table_hbm, table, sems.at[1])
    get_emb.start()
    get_table.start()

    near = nearest[...]
    dest = target[...]
    low = mask(iota((LANES, rows), 0) == (near & (LANES - 1))).astype(BF16)
    looked = dot(keep[...], low)
    kept = jnp.sum(jnp.where(iota(looked.shape, 0) == (near >> 7), looked, 0.0), axis=0, keepdims=True)
    named = jnp.where(iota((shards, rows), 0) == dest, kept, 0.0)
    named_b = named.astype(BF16)
    blk = LANES
    upper = mask((iota((blk, 2 * blk), 0) < iota((blk, 2 * blk), 1)) | (iota((blk, 2 * blk), 1) >= blk)).astype(BF16)
    before = jnp.zeros((shards, blk), F32)
    ranks = []
    for b in range(rows // blk):
        cut = slice(b * blk, (b + 1) * blk)
        both = dot(named_b[:, cut], upper)
        ranks.append(jnp.sum((both[:, :blk] + before) * named[:, cut], axis=0, keepdims=True))
        before = before + both[:, blk:]
    rank = jnp.concatenate(ranks, axis=1).astype(jnp.int32)
    counts = dot(jnp.ones((8, rows), BF16), named_b, NT)[:1]
    slot = jnp.where(kept > 0.5, 8 * dest + rank, -1)

    get_emb.wait()
    squares = []
    for b in range(rows // blk):
        part = emb[b * blk : (b + 1) * blk, :]
        gram = dot(part, part, NT)
        diag = iota((blk, blk), 0) == iota((blk, blk), 1)
        squares.append(jnp.sum(jnp.where(diag, gram, 0.0), axis=0, keepdims=True))
    inverse_row = lax.rsqrt(jnp.concatenate(squares, axis=1) + 1e-06)

    get_table.wait()
    given = jnp.zeros((1, rows), F32)
    others = jnp.full((1, rows), -jnp.inf, F32)
    for c in range(0, classes, CHUNK):
        size = min(CHUNK, classes - c)
        part = table[c : c + size, :]
        wide = part.astype(F32)
        inverse_class = lax.rsqrt(jnp.sum(wide * wide, axis=1, keepdims=True) + 1e-06)
        scaled = dot(part, emb[...], NT) * inverse_class
        match = (iota((size, rows), 0) + c) == near
        given = given + jnp.sum(jnp.where(match, scaled, 0.0), axis=0, keepdims=True)
        others = jnp.maximum(others, jnp.max(jnp.where(match, -1e30, scaled), axis=0, keepdims=True))
    score = (20.0 * (given - others) * inverse_row).astype(BF16).astype(F32)
    lane = (rank + cap * me[0]) & (LANES - 1)
    spread = jnp.where(iota((LANES, rows), 0) == lane, score, 0.0).astype(BF16)
    scores = dot(named_b, spread, NT)

    step = 256
    for g in range(0, 8 * shards, step):
        pick = mask((iota((step, rows), 0) + g) == slot).astype(BF16)
        main = dot(pick, emb[...])
        tail = main[:, head:]
        sub = iota((step, LANES), 0) & 7
        t0 = g // 8
        wide = (step // 8, 8, LANES)
        last = [
            pltpu.roll(tail, 2, 0),
            jnp.broadcast_to(counts, (step, LANES)),
            jnp.broadcast_to(scores[t0 : t0 + step // 8][:, None, :], wide).reshape(step, LANES),
            jnp.broadcast_to(before[t0 : t0 + step // 8][:, None, :], wide).reshape(step, LANES),
            jnp.zeros((step, LANES), F32),
        ]
        for k in range(head // LANES):
            piece = jnp.where(sub < 6, main[:, k * LANES : (k + 1) * LANES], last[k])
            piece = jnp.where(sub == 6, pltpu.roll(tail, 6 - k, 0), piece)
            out[g : g + step, k * LANES : (k + 1) * LANES] = piece.astype(BF16)


def unpack_kernel(got, out_rows, out_score, out_position, out_totals, extra):
    b = pl.program_id(0)
    m, width = out_rows.shape
    k = m // 6 * 8
    head = got.shape[1]
    row, col = iota((m, k), 0), iota((m, k), 1)
    source = (row * 10923) >> 16
    slot = row - 6 * source
    block = got[pl.ds(pl.multiple_of(b * k, k), k), :]
    pick = mask(col == 8 * source + slot).astype(BF16)
    out_rows[:, :head] = dot(pick, block).astype(BF16)
    tail = jnp.zeros((m, width - head), F32)
    for t in range(head // LANES):
        hit = (slot == t) & (col == 8 * source + 6)
        if t == 0:
            hit = hit | ((slot == 5) & (col == 8 * source + 7))
        tail = tail + dot(mask(hit).astype(BF16), block[:, t * LANES : (t + 1) * LANES])
    out_rows[:, head:] = tail.astype(BF16)

    @pl.when(b == 0)
    def _():
        shards = got.shape[0] // 8
        for t in range(3):
            extra[t] = got[:, (t + 1) * LANES : (t + 2) * LANES].astype(F32)
        counts, scores, own = (extra[t, pl.ds(7, shards, stride=8), :] for t in range(3))
        out_totals[...] = jnp.sum(counts, axis=0, keepdims=True).astype(jnp.int32)
        s = iota((shards, LANES), 0)
        for a in range(out_score.shape[0]):
            at = a * LANES + iota((1, LANES), 1)
            src = (at * 10923) >> 16
            j = at - 6 * src
            here = s == src
            score = jnp.sum(jnp.where(here, scores, 0.0), axis=0, keepdims=True)
            held = jnp.sum(jnp.where(here, own, 0.0), axis=0, keepdims=True).astype(jnp.int32)
            ahead = jnp.sum(jnp.where(s < src, own, 0.0), axis=0, keepdims=True).astype(jnp.int32)
            out_score[a : a + 1, :] = score.astype(BF16)
            out_position[a : a + 1, :] = jnp.where(j < held, ahead + j, -1)


def on_device(embeddings, class_table, nearest, keep_class, destination):
    shards = lax.axis_size(GROUP)
    rows, width = embeddings.shape
    cap = 3 * rows // (2 * shards)
    classes = class_table.shape[0]
    head = width - LANES
    me = lax.axis_index(GROUP).reshape(1)
    keep = jnp.pad(keep_class, (0, 8 * LANES - classes)).reshape(8, LANES).astype(BF16)
    vmem = pl.BlockSpec(memory_space=pltpu.VMEM)
    sent = pl.pallas_call(
        pack_kernel,
        in_specs=[
            pl.BlockSpec(memory_space=pltpu.SMEM),
            vmem,
            vmem,
            vmem,
            pl.BlockSpec(memory_space=pl.ANY),
            pl.BlockSpec(memory_space=pl.ANY),
        ],
        out_specs=vmem,
        out_shape=jax.ShapeDtypeStruct((8 * shards, head), BF16),
        scratch_shapes=[
            pltpu.VMEM((rows, width), BF16),
            pltpu.VMEM((classes, width), BF16),
            pltpu.SemaphoreType.DMA((2,)),
        ],
        name="pack",
    )(me, nearest.reshape(1, rows), keep, destination.reshape(1, rows), embeddings, class_table)
    got = lax.all_to_all(sent.reshape(shards, 8, head), GROUP, 0, 0, tiled=True)
    steps = 4
    slots = shards * cap
    received, score, position, totals = pl.pallas_call(
        unpack_kernel,
        grid=(steps,),
        in_specs=[vmem],
        out_specs=[
            pl.BlockSpec((slots // steps, width), lambda b: (b, 0)),
            pl.BlockSpec((slots // LANES, LANES), lambda b: (0, 0)),
            pl.BlockSpec((slots // LANES, LANES), lambda b: (0, 0)),
            pl.BlockSpec((1, shards), lambda b: (0, 0)),
        ],
        out_shape=[
            jax.ShapeDtypeStruct((slots, width), BF16),
            jax.ShapeDtypeStruct((slots // LANES, LANES), BF16),
            jax.ShapeDtypeStruct((slots // LANES, LANES), jnp.int32),
            jax.ShapeDtypeStruct((1, shards), jnp.int32),
        ],
        scratch_shapes=[pltpu.VMEM((3, 8 * shards, LANES), F32)],
        name="unpack",
    )(got.reshape(8 * shards, head))
    return received, score.reshape(slots), position.reshape(slots), totals.reshape(shards)


def solution(mesh):
    return jax.shard_map(
        on_device,
        mesh=mesh,
        in_specs=(P(ALL, None), P(), P(ALL), P(), P(ALL, None)),
        out_specs=(P(ALL, None), P(ALL), P(ALL), P("groups")),
        check_vma=False,
    )
```

```python
import jax
import jax.numpy as jnp
from jax import lax
from jax.experimental import pallas as pl
from jax.experimental.pallas import tpu as pltpu
from jax.sharding import PartitionSpec as P

GROUP = ("owners", "sub")
ALL = ("groups", "owners", "sub")
LANES = 128
CHUNK = 256
CAP = 6
HALF = CAP // 2
F32 = jnp.float32
BF16 = jnp.bfloat16
NT = (((1,), (1,)), ((), ()))
NN = (((1,), (0,)), ((), ()))


def dot(a, b, dims=NN):
    return lax.dot_general(a, b, dims, preferred_element_type=F32)


def iota(shape, dim):
    return lax.broadcasted_iota(jnp.int32, shape, dim)


def mask(cond):
    return jnp.where(cond, 1.0, 0.0)


def sixth(x):
    return (x * 10923) >> 16


def pack_kernel(me, near_hbm, keep_hbm, dest_hbm, emb_hbm, table_hbm, out, near_v, keep_v, dest_v, emb, table, sems):
    rows, width = emb.shape
    classes = table.shape[0]
    shards = out.shape[0]
    moves = [
        pltpu.make_async_copy(a, b, sems.at[i])
        for i, (a, b) in enumerate(
            [(near_hbm, near_v), (keep_hbm, keep_v), (dest_hbm, dest_v), (emb_hbm, emb), (table_hbm, table)]
        )
    ]
    for move in moves:
        move.start()
    for move in moves[:3]:
        move.wait()

    near = near_v[...]
    dest = dest_v[...]
    full, spare = classes // LANES, classes % LANES
    known = [keep_v[:, i * LANES : (i + 1) * LANES] for i in range(full)]
    if spare:
        known.append(pltpu.roll(keep_v[:, classes - LANES :], spare, 1))
    known.extend([jnp.zeros((1, LANES), jnp.int32)] * (8 - len(known)))
    low = mask(iota((LANES, rows), 0) == (near & (LANES - 1))).astype(BF16)
    looked = dot(jnp.concatenate(known, axis=0).astype(BF16), low)
    kept = jnp.sum(jnp.where(iota(looked.shape, 0) == (near >> 7), looked, 0.0), axis=0, keepdims=True)
    named = jnp.where(iota((shards, rows), 0) == dest, kept, 0.0)
    named_b = named.astype(BF16)
    blk = LANES
    upper = mask((iota((blk, 2 * blk), 0) < iota((blk, 2 * blk), 1)) | (iota((blk, 2 * blk), 1) >= blk)).astype(BF16)
    before = jnp.zeros((shards, blk), F32)
    ranks = []
    for b in range(rows // blk):
        cut = slice(b * blk, (b + 1) * blk)
        both = dot(named_b[:, cut], upper)
        ranks.append(jnp.sum((both[:, :blk] + before) * named[:, cut], axis=0, keepdims=True))
        before = before + both[:, blk:]
    rank = jnp.concatenate(ranks, axis=1).astype(jnp.int32)
    counts = dot(jnp.ones((8, rows), BF16), named_b, NT)[:1]
    slot = jnp.where(kept > 0.5, CAP * dest + rank, -1)
    second = jnp.where(kept > 0.5, 2 * dest + 1, -1)

    moves[3].wait()
    at = 3 * iota((2 * shards, rows), 0)
    pick = jnp.concatenate([mask(at + j == slot).astype(BF16) for j in range(HALF)], axis=0)
    whole = dot(pick, emb[...]).astype(BF16)
    for j in range(HALF):
        piece = whole[2 * shards * j : 2 * shards * (j + 1)]
        out[:, :, j * width : (j + 1) * width] = piece.reshape(shards, 2, width)
    squares = []
    for b in range(rows // blk):
        part = emb[b * blk : (b + 1) * blk, :]
        gram = dot(part, part, NT)
        diag = iota((blk, blk), 0) == iota((blk, blk), 1)
        squares.append(jnp.sum(jnp.where(diag, gram, 0.0), axis=0, keepdims=True))
    inverse_row = lax.rsqrt(jnp.concatenate(squares, axis=1) + 1e-06)

    moves[4].wait()
    given = jnp.zeros((1, rows), F32)
    others = jnp.full((1, rows), -jnp.inf, F32)
    for c in range(0, classes, CHUNK):
        size = min(CHUNK, classes - c)
        part = table[c : c + size, :]
        wide = part.astype(F32)
        inverse_class = lax.rsqrt(jnp.sum(wide * wide, axis=1, keepdims=True) + 1e-06)
        scaled = dot(part, emb[...], NT) * inverse_class
        match = (iota((size, rows), 0) + c) == near
        given = given + jnp.sum(jnp.where(match, scaled, 0.0), axis=0, keepdims=True)
        others = jnp.maximum(others, jnp.max(jnp.where(match, -1e30, scaled), axis=0, keepdims=True))
    score = (20.0 * (given - others) * inverse_row).astype(BF16).astype(F32)
    lane = (rank + CAP * me[0]) & (LANES - 1)
    spread = jnp.where(iota((LANES, rows), 0) == lane, score, 0.0).astype(BF16)
    scores = dot(mask(iota((2 * shards, rows), 0) == second).astype(BF16), spread, NT)
    more = jnp.where((iota((2 * shards, LANES), 0) & 1) == 0, counts, scores).astype(BF16)
    out[:, :, HALF * width :] = more.reshape(shards, 2, LANES)


def unpack_kernel(me, got, rows_hbm, score_hbm, position_hbm, totals_hbm, buf, score_v, position_v, totals_v, extra, sems):
    slots, width = rows_hbm.shape
    shards = got.shape[0]
    steps = sems.shape[0] - 3
    m, q = slots // steps, 2 * shards // steps
    third = (iota((m, m), 0) * 21846) >> 16
    pick = mask(third + q * (iota((m, m), 0) - HALF * third) == iota((m, m), 1)).astype(BF16)
    moves = []

    def start(src, dst):
        move = pltpu.make_async_copy(src, dst, sems.at[len(moves)])
        move.start()
        moves.append(move)

    for b in range(steps):
        block = got[b * (q // 2) : (b + 1) * (q // 2), :, : HALF * width].reshape(q, HALF * width)
        block = jnp.concatenate([block[:, j * width : (j + 1) * width] for j in range(HALF)], axis=0)
        buf[b * m : (b + 1) * m, :] = dot(pick, block).astype(BF16)
        start(buf.at[b * m : (b + 1) * m, :], rows_hbm.at[b * m : (b + 1) * m, :])
        if b != steps - 2:
            continue
        extra[...] = got[:, :, HALF * width :].reshape(2 * shards, LANES).astype(F32)
        counts, scores = extra[pl.ds(0, shards, stride=2), :], extra[pl.ds(1, shards, stride=2), :]
        totals_v[...] = jnp.sum(counts, axis=0, keepdims=True).astype(jnp.int32)
        mine = iota((shards, LANES), 1) == me[0]
        own = jnp.sum(jnp.where(mine, counts, 0.0), axis=1, keepdims=True)
        s = iota((shards, LANES), 0)
        for a in range(slots // LANES):
            at = a * LANES + iota((1, LANES), 1)
            src = sixth(at)
            j = at - CAP * src
            here = s == src
            score = jnp.sum(jnp.where(here, scores, 0.0), axis=0, keepdims=True)
            held = jnp.sum(jnp.where(here, own, 0.0), axis=0, keepdims=True).astype(jnp.int32)
            ahead = jnp.sum(jnp.where(s < src, own, 0.0), axis=0, keepdims=True).astype(jnp.int32)
            score_v[a : a + 1, :] = score.astype(BF16)
            position_v[a : a + 1, :] = jnp.where(j < held, ahead + j, -1)
        start(score_v, score_hbm)
        start(position_v, position_hbm)
        start(totals_v, totals_hbm)
    for move in moves:
        move.wait()


def on_device(embeddings, class_table, nearest, keep_class, destination):
    shards = lax.axis_size(GROUP)
    rows, width = embeddings.shape
    classes = class_table.shape[0]
    chunk = HALF * width + LANES
    me = lax.axis_index(GROUP).reshape(1)
    vmem = pl.BlockSpec(memory_space=pltpu.VMEM)
    smem = pl.BlockSpec(memory_space=pltpu.SMEM)
    hbm = pl.BlockSpec(memory_space=pl.ANY)
    sent = pl.pallas_call(
        pack_kernel,
        in_specs=[smem, hbm, hbm, hbm, hbm, hbm],
        out_specs=vmem,
        out_shape=pltpu.VMEM((shards, 2, chunk), BF16),
        scratch_shapes=[
            pltpu.VMEM((1, rows), jnp.int32),
            pltpu.VMEM((1, classes), jnp.int32),
            pltpu.VMEM((1, rows), jnp.int32),
            pltpu.VMEM((rows, width), BF16),
            pltpu.VMEM((classes, width), BF16),
            pltpu.SemaphoreType.DMA((5,)),
        ],
        name="pack",
    )(me, nearest.reshape(1, rows), keep_class.reshape(1, classes), destination.reshape(1, rows), embeddings, class_table)
    got = lax.all_to_all(sent, GROUP, 0, 0, tiled=True)
    steps = 4
    slots = shards * CAP
    tall = slots // LANES
    received, score, position, totals = pl.pallas_call(
        unpack_kernel,
        in_specs=[smem, vmem],
        out_specs=[hbm, hbm, hbm, hbm],
        out_shape=[
            jax.ShapeDtypeStruct((slots, width), BF16),
            jax.ShapeDtypeStruct((tall, LANES), BF16),
            jax.ShapeDtypeStruct((tall, LANES), jnp.int32),
            jax.ShapeDtypeStruct((1, shards), jnp.int32),
        ],
        scratch_shapes=[
            pltpu.VMEM((slots, width), BF16),
            pltpu.VMEM((tall, LANES), BF16),
            pltpu.VMEM((tall, LANES), jnp.int32),
            pltpu.VMEM((1, shards), jnp.int32),
            pltpu.VMEM((2 * shards, LANES), F32),
            pltpu.SemaphoreType.DMA((steps + 3,)),
        ],
        name="unpack",
    )(me, pltpu.with_memory_space_constraint(got, pltpu.VMEM))
    return received, score.reshape(slots), position.reshape(slots), totals.reshape(shards)


def solution(mesh):
    return jax.shard_map(
        on_device,
        mesh=mesh,
        in_specs=(P(ALL, None), P(), P(ALL), P(), P(ALL, None)),
        out_specs=(P(ALL, None), P(ALL), P(ALL), P("groups")),
        check_vma=False,
    )
```

```python
import functools

import jax
import jax.numpy as jnp
from jax import lax
from jax.experimental import pallas as pl
from jax.experimental.pallas import tpu as pltpu
from jax.sharding import Mesh
from jax.sharding import PartitionSpec as P

CHIPS = ("x", "sub")
GROUP = ("x", "core", "sub")
ALL = ("groups", "x", "core", "sub")
CORES = 2
LANES = 128
CHUNK = 256
CAP = 6
HALF = CAP // 2
F32 = jnp.float32
BF16 = jnp.bfloat16
NT = (((1,), (1,)), ((), ()))
NN = (((1,), (0,)), ((), ()))


def dot(a, b, dims=NN):
    return lax.dot_general(a, b, dims, preferred_element_type=F32)


def iota(shape, dim):
    return lax.broadcasted_iota(jnp.int32, shape, dim)


def mask(cond):
    return jnp.where(cond, 1.0, 0.0)


def sixth(x):
    return (x * 10923) >> 16


def log2(n):
    return n.bit_length() - 1


def pack_kernel(subs, me, near_hbm, keep_hbm, dest_hbm, emb_hbm, table_hbm, out, near_v, keep_v, dest_v, emb, table, sems):
    rows, width = emb.shape
    classes = table.shape[0]
    shards = out.shape[0]
    moves = [
        pltpu.make_async_copy(a, b, sems.at[i])
        for i, (a, b) in enumerate(
            [(near_hbm, near_v), (keep_hbm, keep_v), (dest_hbm, dest_v), (emb_hbm, emb), (table_hbm, table)]
        )
    ]
    for move in moves:
        move.start()
    for move in moves[:3]:
        move.wait()

    near = near_v[...]
    dest = dest_v[...]
    full, spare = classes // LANES, classes % LANES
    known = [keep_v[:, i * LANES : (i + 1) * LANES] for i in range(full)]
    if spare:
        known.append(pltpu.roll(keep_v[:, classes - LANES :], spare, 1))
    known.extend([jnp.zeros((1, LANES), jnp.int32)] * (8 - len(known)))
    low = mask(iota((LANES, rows), 0) == (near & (LANES - 1))).astype(BF16)
    looked = dot(jnp.concatenate(known, axis=0).astype(BF16), low)
    kept = jnp.sum(jnp.where(iota(looked.shape, 0) == (near >> 7), looked, 0.0), axis=0, keepdims=True)
    named = jnp.where(iota((shards, rows), 0) == dest, kept, 0.0)
    named_b = named.astype(BF16)
    blk = LANES
    upper = mask((iota((blk, 2 * blk), 0) < iota((blk, 2 * blk), 1)) | (iota((blk, 2 * blk), 1) >= blk)).astype(BF16)
    before = jnp.zeros((shards, blk), F32)
    ranks = []
    for b in range(rows // blk):
        cut = slice(b * blk, (b + 1) * blk)
        both = dot(named_b[:, cut], upper)
        ranks.append(jnp.sum((both[:, :blk] + before) * named[:, cut], axis=0, keepdims=True))
        before = before + both[:, blk:]
    rank = jnp.concatenate(ranks, axis=1).astype(jnp.int32)
    counts = dot(jnp.ones((8, rows), BF16), named_b, NT)[:1]
    core, y = (dest >> log2(subs)) & 1, dest & (subs - 1)
    away = core ^ ((me[0] >> log2(subs)) & 1)
    place = (dest - core * subs - y) + CORES * y + away
    slot = jnp.where(kept > 0.5, CAP * place + rank, -1)
    second = jnp.where(kept > 0.5, 2 * place + 1, -1)

    moves[3].wait()
    at = 3 * iota((2 * shards, rows), 0)
    pick = jnp.concatenate([mask(at + j == slot).astype(BF16) for j in range(HALF)], axis=0)
    whole = dot(pick, emb[...]).astype(BF16)
    for j in range(HALF):
        piece = whole[2 * shards * j : 2 * shards * (j + 1)]
        out[:, :, j * width : (j + 1) * width] = piece.reshape(shards, 2, width)
    squares = []
    for b in range(rows // blk):
        part = emb[b * blk : (b + 1) * blk, :]
        gram = dot(part, part, NT)
        diag = iota((blk, blk), 0) == iota((blk, blk), 1)
        squares.append(jnp.sum(jnp.where(diag, gram, 0.0), axis=0, keepdims=True))
    inverse_row = lax.rsqrt(jnp.concatenate(squares, axis=1) + 1e-06)

    moves[4].wait()
    given = jnp.zeros((1, rows), F32)
    others = jnp.full((1, rows), -jnp.inf, F32)
    for c in range(0, classes, CHUNK):
        size = min(CHUNK, classes - c)
        part = table[c : c + size, :]
        wide = part.astype(F32)
        inverse_class = lax.rsqrt(jnp.sum(wide * wide, axis=1, keepdims=True) + 1e-06)
        scaled = dot(part, emb[...], NT) * inverse_class
        match = (iota((size, rows), 0) + c) == near
        given = given + jnp.sum(jnp.where(match, scaled, 0.0), axis=0, keepdims=True)
        others = jnp.maximum(others, jnp.max(jnp.where(match, -1e30, scaled), axis=0, keepdims=True))
    score = (20.0 * (given - others) * inverse_row).astype(BF16).astype(F32)
    lane = (rank + CAP * me[0]) & (LANES - 1)
    spread = jnp.where(iota((LANES, rows), 0) == lane, score, 0.0).astype(BF16)
    scores = dot(mask(iota((2 * shards, rows), 0) == second).astype(BF16), spread, NT)
    more = jnp.where((iota((2 * shards, LANES), 0) & 1) == 0, counts, scores).astype(BF16)
    out[:, :, HALF * width :] = more.reshape(shards, 2, LANES)


def unpack_kernel(me, got, passed, rows_hbm, score_hbm, position_hbm, totals_hbm, buf, score_v, position_v, totals_v, extra, sems):
    owners, _, deep, width = rows_hbm.shape
    subs = deep // CAP
    chips = passed.shape[0]
    shards = CORES * chips
    core = (me[0] >> log2(subs)) & 1
    steps = 2
    m, q = CAP * chips // steps, 2 * chips // steps
    third = (iota((m, m), 0) * 21846) >> 16
    pick = mask(third + q * (iota((m, m), 0) - HALF * third) == iota((m, m), 1)).astype(BF16)
    moves = []

    def start(src, dst):
        move = pltpu.make_async_copy(src, dst, sems.at[len(moves)])
        move.start()
        moves.append(move)

    for b in range(2 * steps):
        at = slice(b % steps * (q // 2), (b % steps + 1) * (q // 2))
        block = got[at, 0, :, : HALF * width] if b < steps else passed[at, :, : HALF * width]
        block = block.reshape(q, HALF * width)
        block = jnp.concatenate([block[:, j * width : (j + 1) * width] for j in range(HALF)], axis=0)
        part = owners // steps
        buf[b * part : (b + 1) * part] = dot(pick, block).astype(BF16).reshape(part, deep, width)
        where = core if b < steps else 1 - core
        start(buf.at[b * part : (b + 1) * part], rows_hbm.at[b % steps * part : (b % steps + 1) * part, where])
        if b != 2 * steps - 2:
            continue
        extra[: 2 * chips] = got[:, 0, :, HALF * width :].reshape(2 * chips, LANES).astype(F32)
        extra[2 * chips :] = passed[:, :, HALF * width :].reshape(2 * chips, LANES).astype(F32)
        counts, scores = extra[pl.ds(0, shards, stride=2), :], extra[pl.ds(1, shards, stride=2), :]
        totals_v[...] = jnp.sum(counts, axis=0, keepdims=True).astype(jnp.int32)
        mine = iota((shards, LANES), 1) == me[0]
        own = jnp.sum(jnp.where(mine, counts, 0.0), axis=1, keepdims=True)
        i = iota((shards, LANES), 0)
        x, y = (i & (chips - 1)) >> log2(subs), i & (subs - 1)
        s = (CORES * x + jnp.where(i < chips, core, 1 - core)) * subs + y
        for a in range(CAP * shards // LANES):
            at = a * LANES + iota((1, LANES), 1)
            src = sixth(at)
            j = at - CAP * src
            here = s == src
            score = jnp.sum(jnp.where(here, scores, 0.0), axis=0, keepdims=True)
            held = jnp.sum(jnp.where(here, own, 0.0), axis=0, keepdims=True).astype(jnp.int32)
            ahead = jnp.sum(jnp.where(s < src, own, 0.0), axis=0, keepdims=True).astype(jnp.int32)
            score_v[a : a + 1, :] = score.astype(BF16)
            position_v[a : a + 1, :] = jnp.where(j < held, ahead + j, -1)
        start(score_v, score_hbm)
        start(position_v, position_hbm)
        start(totals_v, totals_hbm)
    for move in moves:
        move.wait()


def on_device(embeddings, class_table, nearest, keep_class, destination):
    shards, chips, owners, subs = (lax.axis_size(a) for a in (GROUP, CHIPS, "x", "sub"))
    rows, width = embeddings.shape
    classes = class_table.shape[0]
    chunk = HALF * width + LANES
    me = lax.axis_index(GROUP).reshape(1)
    vmem = pl.BlockSpec(memory_space=pltpu.VMEM)
    smem = pl.BlockSpec(memory_space=pltpu.SMEM)
    hbm = pl.BlockSpec(memory_space=pl.ANY)
    sent = pl.pallas_call(
        functools.partial(pack_kernel, subs),
        in_specs=[smem, hbm, hbm, hbm, hbm, hbm],
        out_specs=vmem,
        out_shape=pltpu.VMEM((shards, 2, chunk), BF16),
        scratch_shapes=[
            pltpu.VMEM((1, rows), jnp.int32),
            pltpu.VMEM((1, classes), jnp.int32),
            pltpu.VMEM((1, rows), jnp.int32),
            pltpu.VMEM((rows, width), BF16),
            pltpu.VMEM((classes, width), BF16),
            pltpu.SemaphoreType.DMA((5,)),
        ],
        name="pack",
    )(me, nearest.reshape(1, rows), keep_class.reshape(1, classes), destination.reshape(1, rows), embeddings, class_table)
    got = lax.all_to_all(sent.reshape(chips, CORES, 2, chunk), CHIPS, 0, 0, tiled=True)
    passed = lax.ppermute(got[:, 1], "core", [(0, 1), (1, 0)])
    slots = shards * CAP
    tall = slots // LANES
    received, score, position, totals = pl.pallas_call(
        unpack_kernel,
        in_specs=[smem, vmem, vmem],
        out_specs=[hbm, hbm, hbm, hbm],
        out_shape=[
            jax.ShapeDtypeStruct((owners, CORES, CAP * subs, width), BF16),
            jax.ShapeDtypeStruct((tall, LANES), BF16),
            jax.ShapeDtypeStruct((tall, LANES), jnp.int32),
            jax.ShapeDtypeStruct((1, shards), jnp.int32),
        ],
        scratch_shapes=[
            pltpu.VMEM((CORES * owners, CAP * subs, width), BF16),
            pltpu.VMEM((tall, LANES), BF16),
            pltpu.VMEM((tall, LANES), jnp.int32),
            pltpu.VMEM((1, shards), jnp.int32),
            pltpu.VMEM((2 * shards, LANES), F32),
            pltpu.SemaphoreType.DMA((7,)),
        ],
        name="unpack",
    )(me, *(pltpu.with_memory_space_constraint(a, pltpu.VMEM) for a in (got, passed)))
    return received.reshape(slots, width), score.reshape(slots), position.reshape(slots), totals.reshape(shards)


def solution(mesh):
    groups, owners, subs = (mesh.shape[a] for a in ("groups", "owners", "sub"))
    split = Mesh(mesh.devices.reshape(groups, owners // CORES, CORES, subs), ALL)
    return jax.shard_map(
        on_device,
        mesh=split,
        in_specs=(P(ALL, None), P(), P(ALL), P(), P(ALL, None)),
        out_specs=(P(ALL, None), P(ALL), P(ALL), P("groups")),
        check_vma=False,
    )
```

```python
import functools

import jax
import jax.numpy as jnp
from jax import lax
from jax.experimental import pallas as pl
from jax.experimental.pallas import tpu as pltpu
from jax.sharding import Mesh
from jax.sharding import PartitionSpec as P

CHIPS = ("x", "sub")
GROUP = ("x", "core", "sub")
ALL = ("groups", "x", "core", "sub")
CORES = 2
LANES = 128
CHUNK = 256
CAP = 6
HALF = CAP // 2
F32 = jnp.float32
BF16 = jnp.bfloat16
NT = (((1,), (1,)), ((), ()))
NN = (((1,), (0,)), ((), ()))


def dot(a, b, dims=NN):
    return lax.dot_general(a, b, dims, preferred_element_type=F32)


def iota(shape, dim):
    return lax.broadcasted_iota(jnp.int32, shape, dim)


def mask(cond):
    return jnp.where(cond, 1.0, 0.0)


def sixth(x):
    return (x * 10923) >> 16


def log2(n):
    return n.bit_length() - 1


def pack_kernel(subs, me, near_hbm, keep_hbm, dest_hbm, emb_hbm, table_hbm, out, near_v, keep_v, dest_v, emb, table, sems):
    rows, width = emb.shape
    classes = table.shape[0]
    chips = out.shape[0]
    shards = CORES * chips
    starts = range(0, classes, CHUNK)
    pairs = [(near_hbm, near_v), (keep_hbm, keep_v), (dest_hbm, dest_v)]
    for r in range(0, rows, rows):
        pairs.append((emb_hbm.at[r : r + rows], emb.at[r : r + rows]))
    for c in starts:
        size = min(CHUNK, classes - c)
        pairs.append((table_hbm.at[c : c + size], table.at[c : c + size]))
    moves = [pltpu.make_async_copy(a, b, sems.at[i]) for i, (a, b) in enumerate(pairs)]
    for move in moves:
        move.start()
    for move in moves[:3]:
        move.wait()

    near = near_v[...]
    dest = dest_v[...]
    full, spare = classes // LANES, classes % LANES
    known = [keep_v[:, i * LANES : (i + 1) * LANES] for i in range(full)]
    if spare:
        known.append(pltpu.roll(keep_v[:, classes - LANES :], spare, 1))
    known.extend([jnp.zeros((1, LANES), jnp.int32)] * (8 - len(known)))
    low = mask(iota((LANES, rows), 0) == (near & (LANES - 1))).astype(BF16)
    looked = dot(jnp.concatenate(known, axis=0).astype(BF16), low)
    kept = jnp.sum(jnp.where(iota(looked.shape, 0) == (near >> 7), looked, 0.0), axis=0, keepdims=True)
    named = jnp.where(iota((shards, rows), 0) == dest, kept, 0.0)
    named_b = named.astype(BF16)
    blk = LANES
    upper = mask((iota((blk, 2 * blk), 0) < iota((blk, 2 * blk), 1)) | (iota((blk, 2 * blk), 1) >= blk)).astype(BF16)
    before = jnp.zeros((shards, blk), F32)
    ranks = []
    for b in range(rows // blk):
        cut = slice(b * blk, (b + 1) * blk)
        both = dot(named_b[:, cut], upper)
        ranks.append(jnp.sum((both[:, :blk] + before) * named[:, cut], axis=0, keepdims=True))
        before = before + both[:, blk:]
    rank = jnp.concatenate(ranks, axis=1).astype(jnp.int32)
    counts = dot(jnp.ones((8, rows), BF16), named_b, NT)[:1]
    core, y = (dest >> log2(subs)) & 1, dest & (subs - 1)
    away = core ^ ((me[0] >> log2(subs)) & 1)
    chip = ((dest - core * subs - y) >> 1) + y
    slot = jnp.where(kept > 0.5, CAP * (away * chips + chip) + rank, -1)
    second = jnp.where(kept > 0.5, 2 * chip + 1, -1)
    at = 3 * iota((2 * shards, rows), 0)

    def place(j):
        picked = dot(mask(at == slot - j).astype(BF16), emb[...]).astype(BF16)
        for k in range(CORES):
            piece = picked[2 * chips * k : 2 * chips * (k + 1)].reshape(chips, 2, width)
            out[:, :, (HALF * k + j) * width : (HALF * k + j + 1) * width] = piece

    def class_scale(c):
        wide = table[c : min(c + CHUNK, classes), :].astype(F32)
        return lax.rsqrt(jnp.sum(wide * wide, axis=1, keepdims=True) + 1e-06)

    for move in moves[3:4]:
        move.wait()
    place(0)
    place(1)
    squares = []
    for b in range(rows // blk):
        part = emb[b * blk : (b + 1) * blk, :]
        gram = dot(part, part, NT)
        diag = iota((blk, blk), 0) == iota((blk, blk), 1)
        squares.append(jnp.sum(jnp.where(diag, gram, 0.0), axis=0, keepdims=True))
    inverse_row = lax.rsqrt(jnp.concatenate(squares, axis=1) + 1e-06)
    for move in moves[4:]:
        move.wait()
    inverse_class = {}
    given = jnp.zeros((1, rows), F32)
    others = jnp.full((1, rows), -jnp.inf, F32)
    for c in starts:
        size = min(CHUNK, classes - c)
        inverse_class[c] = class_scale(c)
        scaled = dot(table[c : c + size, :], emb[...], NT) * inverse_class[c]
        match = iota((size, rows), 0) == near - c
        given = given + jnp.sum(jnp.where(match, scaled, 0.0), axis=0, keepdims=True)
        others = jnp.maximum(others, jnp.max(jnp.where(match, -1e30, scaled), axis=0, keepdims=True))
    score = (20.0 * (given - others) * inverse_row).astype(BF16).astype(F32)
    lane = (rank + CAP * me[0] + LANES // CORES * away) & (LANES - 1)
    spread = jnp.where(iota((LANES, rows), 0) == lane, score, 0.0).astype(BF16)
    place(2)
    scores = dot(mask(iota((2 * chips, rows), 0) == second).astype(BF16), spread, NT)
    more = jnp.where((iota((2 * chips, LANES), 0) & 1) == 0, counts, scores).astype(BF16)
    out[:, :, CAP * width :] = more.reshape(chips, 2, LANES)


def unpack_half(src, side, buf, rows_hbm, sems, between=None):
    owners, _, deep, width = rows_hbm.shape
    chips = owners * deep // CAP
    steps = sems.shape[0]
    m, q, part = CAP * chips // steps, 2 * chips // steps, owners // steps
    third = (iota((m, m), 0) * 21846) >> 16
    pick = mask(third + q * (iota((m, m), 0) - HALF * third) == iota((m, m), 1)).astype(BF16)
    moves = []
    for b in range(steps):
        if between and b == steps - 1:
            between()
        block = src(b * (q // 2), (b + 1) * (q // 2)).reshape(q, HALF * width)
        block = jnp.concatenate([block[:, j * width : (j + 1) * width] for j in range(HALF)], axis=0)
        cut = slice(b * part, (b + 1) * part)
        buf[cut] = dot(pick, block).astype(BF16).reshape(part, deep, width)
        move = pltpu.make_async_copy(buf.at[cut], rows_hbm.at[cut, side], sems.at[b])
        move.start()
        moves.append(move)
    return moves


def own_kernel(me, got, rows_hbm, buf, sems):
    subs, width = rows_hbm.shape[2] // CAP, rows_hbm.shape[3]
    core = (me[0] >> log2(subs)) & 1
    for move in unpack_half(lambda a, b: got[a:b, :, : HALF * width], core, buf, rows_hbm, sems):
        move.wait()


def passed_kernel(
    me, got, passed, own_rows, rows_hbm, score_hbm, position_hbm, totals_hbm, buf, score_v, position_v, totals_v, extra, sems, late
):
    del own_rows
    subs, width = rows_hbm.shape[2] // CAP, rows_hbm.shape[3]
    chips = passed.shape[0]
    shards = CORES * chips
    core = (me[0] >> log2(subs)) & 1
    results = [(score_v, score_hbm), (position_v, position_hbm), (totals_v, totals_hbm)]
    small = [pltpu.make_async_copy(a, b, late.at[i]) for i, (a, b) in enumerate(results)]

    def between():
        extra[: 2 * chips] = got[:, :, CAP * width :].reshape(2 * chips, LANES).astype(F32)
        extra[2 * chips :] = passed[:, :, HALF * width :].reshape(2 * chips, LANES).astype(F32)
        counts, scores = extra[pl.ds(0, shards, stride=2), :], extra[pl.ds(1, shards, stride=2), :]
        scores = jnp.concatenate([scores[:chips], pltpu.roll(scores[chips:], LANES // CORES, 1)], axis=0)
        totals_v[...] = jnp.sum(counts, axis=0, keepdims=True).astype(jnp.int32)
        lane = iota((shards, LANES), 1) == me[0]
        own = jnp.sum(jnp.where(lane, counts, 0.0), axis=1, keepdims=True)
        i = iota((shards, LANES), 0)
        x, y = (i & (chips - 1)) >> log2(subs), i & (subs - 1)
        s = (CORES * x + jnp.where(i < chips, core, 1 - core)) * subs + y
        for a in range(CAP * shards // LANES):
            at = a * LANES + iota((1, LANES), 1)
            src = sixth(at)
            j = at - CAP * src
            here = s == src
            score = jnp.sum(jnp.where(here, scores, 0.0), axis=0, keepdims=True)
            held = jnp.sum(jnp.where(here, own, 0.0), axis=0, keepdims=True).astype(jnp.int32)
            ahead = jnp.sum(jnp.where(s < src, own, 0.0), axis=0, keepdims=True).astype(jnp.int32)
            score_v[a : a + 1, :] = score.astype(BF16)
            position_v[a : a + 1, :] = jnp.where(j < held, ahead + j, -1)
        for move in small:
            move.start()

    moves = unpack_half(lambda a, b: passed[a:b, :, : HALF * width], 1 - core, buf, rows_hbm, sems, between)
    for move in moves + small:
        move.wait()


def on_device(embeddings, class_table, nearest, keep_class, destination):
    shards, chips, owners, subs = (lax.axis_size(a) for a in (GROUP, CHIPS, "x", "sub"))
    rows, width = embeddings.shape
    classes = class_table.shape[0]
    chunk = CAP * width + LANES
    me = lax.axis_index(GROUP).reshape(1)
    vmem = pl.BlockSpec(memory_space=pltpu.VMEM)
    smem = pl.BlockSpec(memory_space=pltpu.SMEM)
    hbm = pl.BlockSpec(memory_space=pl.ANY)
    sent = pl.pallas_call(
        functools.partial(pack_kernel, subs),
        in_specs=[smem, hbm, hbm, hbm, hbm, hbm],
        out_specs=vmem,
        out_shape=pltpu.VMEM((chips, 2, chunk), BF16),
        scratch_shapes=[
            pltpu.VMEM((1, rows), jnp.int32),
            pltpu.VMEM((1, classes), jnp.int32),
            pltpu.VMEM((1, rows), jnp.int32),
            pltpu.VMEM((rows, width), BF16),
            pltpu.VMEM((classes, width), BF16),
            pltpu.SemaphoreType.DMA((4 + pl.cdiv(classes, CHUNK),)),
        ],
        name="pack",
    )(me, nearest.reshape(1, rows), keep_class.reshape(1, classes), destination.reshape(1, rows), embeddings, class_table)
    got = lax.all_to_all(sent, CHIPS, 0, 0, tiled=True)
    passed = lax.ppermute(got[:, :, HALF * width :], "core", [(0, 1), (1, 0)])
    slots = shards * CAP
    tall = slots // LANES
    rows_shape = jax.ShapeDtypeStruct((owners, CORES, CAP * subs, width), BF16)
    buf = pltpu.VMEM((owners, CAP * subs, width), BF16)
    got = pltpu.with_memory_space_constraint(got, pltpu.VMEM)
    own_rows = pl.pallas_call(
        own_kernel,
        in_specs=[smem, vmem],
        out_specs=hbm,
        out_shape=rows_shape,
        scratch_shapes=[buf, pltpu.SemaphoreType.DMA((2,))],
        name="own",
    )(me, got)
    received, score, position, totals = pl.pallas_call(
        passed_kernel,
        in_specs=[smem, vmem, vmem, hbm],
        out_specs=[hbm, hbm, hbm, hbm],
        out_shape=[
            rows_shape,
            jax.ShapeDtypeStruct((tall, LANES), BF16),
            jax.ShapeDtypeStruct((tall, LANES), jnp.int32),
            jax.ShapeDtypeStruct((1, shards), jnp.int32),
        ],
        scratch_shapes=[
            buf,
            pltpu.VMEM((tall, LANES), BF16),
            pltpu.VMEM((tall, LANES), jnp.int32),
            pltpu.VMEM((1, shards), jnp.int32),
            pltpu.VMEM((2 * shards, LANES), F32),
            pltpu.SemaphoreType.DMA((2,)),
            pltpu.SemaphoreType.DMA((3,)),
        ],
        input_output_aliases={3: 0},
        name="passed",
    )(me, got, pltpu.with_memory_space_constraint(passed, pltpu.VMEM), own_rows)
    return received.reshape(slots, width), score.reshape(slots), position.reshape(slots), totals.reshape(shards)


def solution(mesh):
    groups, owners, subs = (mesh.shape[a] for a in ("groups", "owners", "sub"))
    split = Mesh(mesh.devices.reshape(groups, owners // CORES, CORES, subs), ALL)
    return jax.shard_map(
        on_device,
        mesh=split,
        in_specs=(P(ALL, None), P(), P(ALL), P(), P(ALL, None)),
        out_specs=(P(ALL, None), P(ALL), P(ALL), P("groups")),
        check_vma=False,
    )
```

```python
import functools

import jax
import jax.numpy as jnp
from jax import lax
from jax.experimental import pallas as pl
from jax.experimental.pallas import tpu as pltpu
from jax.sharding import Mesh
from jax.sharding import PartitionSpec as P

CHIPS = ("x", "sub")
GROUP = ("x", "core", "sub")
ALL = ("groups", "x", "core", "sub")
CORES = 2
LANES = 128
CHUNK = 1024
CAP = 6
HALF = CAP // 2
F32 = jnp.float32
BF16 = jnp.bfloat16
NT = (((1,), (1,)), ((), ()))
NN = (((1,), (0,)), ((), ()))


def dot(a, b, dims=NN):
    return lax.dot_general(a, b, dims, preferred_element_type=F32)


def iota(shape, dim):
    return lax.broadcasted_iota(jnp.int32, shape, dim)


def mask(cond):
    return jnp.where(cond, 1.0, 0.0)


def sixth(x):
    return (x * 10923) >> 16


def log2(n):
    return n.bit_length() - 1


def pack_kernel(subs, me, near_hbm, keep_hbm, dest_hbm, emb_hbm, table_hbm, out, near_v, keep_v, dest_v, emb, table, sems):
    rows, width = emb.shape
    classes = table.shape[0]
    chips = out.shape[0]
    shards = CORES * chips
    starts = range(0, classes, CHUNK)
    pairs = [(near_hbm, near_v), (keep_hbm, keep_v), (dest_hbm, dest_v)]
    for r in range(0, rows, rows):
        pairs.append((emb_hbm.at[r : r + rows], emb.at[r : r + rows]))
    for c in starts:
        size = min(CHUNK, classes - c)
        pairs.append((table_hbm.at[c : c + size], table.at[c : c + size]))
    moves = [pltpu.make_async_copy(a, b, sems.at[i]) for i, (a, b) in enumerate(pairs)]
    for move in moves:
        move.start()
    for move in moves[:3]:
        move.wait()

    near = near_v[...]
    dest = dest_v[...]
    full, spare = classes // LANES, classes % LANES
    known = [keep_v[:, i * LANES : (i + 1) * LANES] for i in range(full)]
    if spare:
        known.append(pltpu.roll(keep_v[:, classes - LANES :], spare, 1))
    known.extend([jnp.zeros((1, LANES), jnp.int32)] * (8 - len(known)))
    low = mask(iota((LANES, rows), 0) == (near & (LANES - 1))).astype(BF16)
    looked = dot(jnp.concatenate(known, axis=0).astype(BF16), low)
    kept = jnp.sum(jnp.where(iota(looked.shape, 0) == (near >> 7), looked, 0.0), axis=0, keepdims=True)
    named = jnp.where(iota((shards, rows), 0) == dest, kept, 0.0)
    named_b = named.astype(BF16)
    blk = LANES
    upper = mask((iota((blk, 2 * blk), 0) < iota((blk, 2 * blk), 1)) | (iota((blk, 2 * blk), 1) >= blk)).astype(BF16)
    before = jnp.zeros((shards, blk), F32)
    ranks = []
    for b in range(rows // blk):
        cut = slice(b * blk, (b + 1) * blk)
        both = dot(named_b[:, cut], upper)
        ranks.append(jnp.sum((both[:, :blk] + before) * named[:, cut], axis=0, keepdims=True))
        before = before + both[:, blk:]
    rank = jnp.concatenate(ranks, axis=1).astype(jnp.int32)
    counts = dot(jnp.ones((8, rows), BF16), named_b, NT)[:1]
    core, y = (dest >> log2(subs)) & 1, dest & (subs - 1)
    away = core ^ ((me[0] >> log2(subs)) & 1)
    chip = ((dest - core * subs - y) >> 1) + y
    slot = jnp.where(kept > 0.5, CAP * (away * chips + chip) + rank, -1)
    second = jnp.where(kept > 0.5, 2 * chip + 1, -1)
    at = 3 * iota((2 * shards, rows), 0)

    def place(j):
        picked = dot(mask(at == slot - j).astype(BF16), emb[...]).astype(BF16)
        for k in range(CORES):
            piece = picked[2 * chips * k : 2 * chips * (k + 1)].reshape(chips, 2, width)
            out[:, :, (HALF * k + j) * width : (HALF * k + j + 1) * width] = piece

    def class_scale(c):
        wide = table[c : min(c + CHUNK, classes), :].astype(F32)
        return lax.rsqrt(jnp.sum(wide * wide, axis=1, keepdims=True) + 1e-06)

    for move in moves[3:4]:
        move.wait()
    place(0)
    place(1)
    squares = []
    for b in range(rows // blk):
        part = emb[b * blk : (b + 1) * blk, :]
        gram = dot(part, part, NT)
        diag = iota((blk, blk), 0) == iota((blk, blk), 1)
        squares.append(jnp.sum(jnp.where(diag, gram, 0.0), axis=0, keepdims=True))
    inverse_row = lax.rsqrt(jnp.concatenate(squares, axis=1) + 1e-06)
    for move in moves[4:]:
        move.wait()
    inverse_class = {}
    given = jnp.zeros((1, rows), F32)
    others = jnp.full((1, rows), -jnp.inf, F32)
    for c in starts:
        size = min(CHUNK, classes - c)
        inverse_class[c] = class_scale(c)
        scaled = dot(table[c : c + size, :], emb[...], NT) * inverse_class[c]
        match = iota((size, rows), 0) == near - c
        given = given + jnp.sum(jnp.where(match, scaled, 0.0), axis=0, keepdims=True)
        others = jnp.maximum(others, jnp.max(jnp.where(match, -1e30, scaled), axis=0, keepdims=True))
    score = (20.0 * (given - others) * inverse_row).astype(BF16).astype(F32)
    lane = (rank + CAP * me[0] + LANES // CORES * away) & (LANES - 1)
    spread = jnp.where(iota((LANES, rows), 0) == lane, score, 0.0).astype(BF16)
    place(2)
    scores = dot(mask(iota((2 * chips, rows), 0) == second).astype(BF16), spread, NT)
    more = jnp.where((iota((2 * chips, LANES), 0) & 1) == 0, counts, scores).astype(BF16)
    out[:, :, CAP * width :] = more.reshape(chips, 2, LANES)


def unpack_half(src, side, buf, rows_hbm, sems, between=None):
    owners, _, deep, width = rows_hbm.shape
    chips = owners * deep // CAP
    steps = sems.shape[0]
    m, q, part = CAP * chips // steps, 2 * chips // steps, owners // steps
    third = (iota((m, m), 0) * 21846) >> 16
    pick = mask(third + q * (iota((m, m), 0) - HALF * third) == iota((m, m), 1)).astype(BF16)
    moves = []
    for b in range(steps):
        if between and b == steps - 1:
            between()
        block = src(b * (q // 2), (b + 1) * (q // 2)).reshape(q, HALF * width)
        block = jnp.concatenate([block[:, j * width : (j + 1) * width] for j in range(HALF)], axis=0)
        cut = slice(b * part, (b + 1) * part)
        buf[cut] = dot(pick, block).astype(BF16).reshape(part, deep, width)
        move = pltpu.make_async_copy(buf.at[cut], rows_hbm.at[cut, side], sems.at[b])
        move.start()
        moves.append(move)
    return moves


def part_kernel(got, out):
    chips, _, chunk = out.shape
    for at in range(0, chunk, LANES):
        skip = got.shape[2] - chunk + at
        out[:, :, at : at + LANES] = got[:, :, skip : skip + LANES].reshape(2 * chips, LANES).reshape(chips, 2, LANES)


def own_kernel(me, got, rows_hbm, buf, sems):
    subs, width = rows_hbm.shape[2] // CAP, rows_hbm.shape[3]
    core = (me[0] >> log2(subs)) & 1
    for move in unpack_half(lambda a, b: got[a:b, :, : HALF * width], core, buf, rows_hbm, sems):
        move.wait()


def passed_kernel(
    me, got, passed, own_rows, rows_hbm, score_hbm, position_hbm, totals_hbm, buf, score_v, position_v, totals_v, extra, sems, late
):
    del own_rows
    subs, width = rows_hbm.shape[2] // CAP, rows_hbm.shape[3]
    chips = passed.shape[0]
    shards = CORES * chips
    core = (me[0] >> log2(subs)) & 1
    results = [(score_v, score_hbm), (position_v, position_hbm), (totals_v, totals_hbm)]
    small = [pltpu.make_async_copy(a, b, late.at[i]) for i, (a, b) in enumerate(results)]

    def between():
        extra[: 2 * chips] = got[:, :, CAP * width :].reshape(2 * chips, LANES).astype(F32)
        extra[2 * chips :] = passed[:, :, HALF * width :].reshape(2 * chips, LANES).astype(F32)
        counts, scores = extra[pl.ds(0, shards, stride=2), :], extra[pl.ds(1, shards, stride=2), :]
        scores = jnp.concatenate([scores[:chips], pltpu.roll(scores[chips:], LANES // CORES, 1)], axis=0)
        totals_v[...] = jnp.sum(counts, axis=0, keepdims=True).astype(jnp.int32)
        lane = iota((shards, LANES), 1) == me[0]
        own = jnp.sum(jnp.where(lane, counts, 0.0), axis=1, keepdims=True)
        i = iota((shards, LANES), 0)
        x, y = (i & (chips - 1)) >> log2(subs), i & (subs - 1)
        s = (CORES * x + jnp.where(i < chips, core, 1 - core)) * subs + y
        for a in range(CAP * shards // LANES):
            at = a * LANES + iota((1, LANES), 1)
            src = sixth(at)
            j = at - CAP * src
            here = s == src
            score = jnp.sum(jnp.where(here, scores, 0.0), axis=0, keepdims=True)
            held = jnp.sum(jnp.where(here, own, 0.0), axis=0, keepdims=True).astype(jnp.int32)
            ahead = jnp.sum(jnp.where(s < src, own, 0.0), axis=0, keepdims=True).astype(jnp.int32)
            score_v[a : a + 1, :] = score.astype(BF16)
            position_v[a : a + 1, :] = jnp.where(j < held, ahead + j, -1)
        for move in small:
            move.start()

    moves = unpack_half(lambda a, b: passed[a:b, :, : HALF * width], 1 - core, buf, rows_hbm, sems, between)
    for move in moves + small:
        move.wait()


def on_device(embeddings, class_table, nearest, keep_class, destination):
    shards, chips, owners, subs = (lax.axis_size(a) for a in (GROUP, CHIPS, "x", "sub"))
    rows, width = embeddings.shape
    classes = class_table.shape[0]
    chunk = CAP * width + LANES
    me = lax.axis_index(GROUP).reshape(1)
    vmem = pl.BlockSpec(memory_space=pltpu.VMEM)
    smem = pl.BlockSpec(memory_space=pltpu.SMEM)
    hbm = pl.BlockSpec(memory_space=pl.ANY)
    sent = pl.pallas_call(
        functools.partial(pack_kernel, subs),
        in_specs=[smem, hbm, hbm, hbm, hbm, hbm],
        out_specs=vmem,
        out_shape=pltpu.VMEM((chips, 2, chunk), BF16),
        scratch_shapes=[
            pltpu.VMEM((1, rows), jnp.int32),
            pltpu.VMEM((1, classes), jnp.int32),
            pltpu.VMEM((1, rows), jnp.int32),
            pltpu.VMEM((rows, width), BF16),
            pltpu.VMEM((classes, width), BF16),
            pltpu.SemaphoreType.DMA((4 + pl.cdiv(classes, CHUNK),)),
        ],
        name="pack",
    )(me, nearest.reshape(1, rows), keep_class.reshape(1, classes), destination.reshape(1, rows), embeddings, class_table)
    got = lax.all_to_all(sent, CHIPS, 0, 0, tiled=True)
    got = pltpu.with_memory_space_constraint(got, pltpu.VMEM)
    passed = pl.pallas_call(
        part_kernel,
        in_specs=[vmem],
        out_specs=vmem,
        out_shape=pltpu.VMEM((chips, 2, HALF * width + LANES), BF16),
        name="part",
    )(got)
    passed = lax.ppermute(passed, "core", [(0, 1), (1, 0)])
    slots = shards * CAP
    tall = slots // LANES
    rows_shape = jax.ShapeDtypeStruct((owners, CORES, CAP * subs, width), BF16)
    buf = pltpu.VMEM((owners, CAP * subs, width), BF16)
    own_rows = pl.pallas_call(
        own_kernel,
        in_specs=[smem, vmem],
        out_specs=hbm,
        out_shape=rows_shape,
        scratch_shapes=[buf, pltpu.SemaphoreType.DMA((2,))],
        name="own",
    )(me, got)
    received, score, position, totals = pl.pallas_call(
        passed_kernel,
        in_specs=[smem, vmem, vmem, hbm],
        out_specs=[hbm, hbm, hbm, hbm],
        out_shape=[
            rows_shape,
            jax.ShapeDtypeStruct((tall, LANES), BF16),
            jax.ShapeDtypeStruct((tall, LANES), jnp.int32),
            jax.ShapeDtypeStruct((1, shards), jnp.int32),
        ],
        scratch_shapes=[
            buf,
            pltpu.VMEM((tall, LANES), BF16),
            pltpu.VMEM((tall, LANES), jnp.int32),
            pltpu.VMEM((1, shards), jnp.int32),
            pltpu.VMEM((2 * shards, LANES), F32),
            pltpu.SemaphoreType.DMA((2,)),
            pltpu.SemaphoreType.DMA((3,)),
        ],
        input_output_aliases={3: 0},
        name="passed",
    )(me, got, pltpu.with_memory_space_constraint(passed, pltpu.VMEM), own_rows)
    return received.reshape(slots, width), score.reshape(slots), position.reshape(slots), totals.reshape(shards)


def solution(mesh):
    groups, owners, subs = (mesh.shape[a] for a in ("groups", "owners", "sub"))
    split = Mesh(mesh.devices.reshape(groups, owners // CORES, CORES, subs), ALL)
    return jax.shard_map(
        on_device,
        mesh=split,
        in_specs=(P(ALL, None), P(), P(ALL), P(), P(ALL, None)),
        out_specs=(P(ALL, None), P(ALL), P(ALL), P("groups")),
        check_vma=False,
    )
```

```python
import functools

import jax
import jax.numpy as jnp
from jax import lax
from jax.experimental import pallas as pl
from jax.experimental.pallas import tpu as pltpu
from jax.sharding import Mesh
from jax.sharding import PartitionSpec as P

CHIPS = ("x", "sub")
GROUP = ("x", "core", "sub")
ALL = ("groups", "x", "core", "sub")
CORES = 2
LANES = 128
CHUNK = 1024
CAP = 6
HALF = CAP // 2
F32 = jnp.float32
BF16 = jnp.bfloat16
NT = (((1,), (1,)), ((), ()))
NN = (((1,), (0,)), ((), ()))


def dot(a, b, dims=NN):
    return lax.dot_general(a, b, dims, preferred_element_type=F32)


def iota(shape, dim):
    return lax.broadcasted_iota(jnp.int32, shape, dim)


def mask(cond):
    return jnp.where(cond, 1.0, 0.0)


def sixth(x):
    return (x * 10923) >> 16


def log2(n):
    return n.bit_length() - 1


def pack_kernel(subs, me, near_hbm, keep_hbm, dest_hbm, emb_hbm, table_hbm, out, near_v, keep_v, dest_v, emb, table, sems):
    rows, width = emb.shape
    classes = table.shape[0]
    chips = out.shape[0]
    shards = CORES * chips
    starts = range(0, classes, CHUNK)
    pairs = [(near_hbm, near_v), (keep_hbm, keep_v), (dest_hbm, dest_v)]
    for r in range(0, rows, rows):
        pairs.append((emb_hbm.at[r : r + rows], emb.at[r : r + rows]))
    for c in starts:
        size = min(CHUNK, classes - c)
        pairs.append((table_hbm.at[c : c + size], table.at[c : c + size]))
    moves = [pltpu.make_async_copy(a, b, sems.at[i]) for i, (a, b) in enumerate(pairs)]
    for move in moves:
        move.start()
    for move in moves[:3]:
        move.wait()

    near = near_v[...]
    dest = dest_v[...]
    full, spare = classes // LANES, classes % LANES
    known = [keep_v[:, i * LANES : (i + 1) * LANES] for i in range(full)]
    if spare:
        known.append(pltpu.roll(keep_v[:, classes - LANES :], spare, 1))
    known.extend([jnp.zeros((1, LANES), jnp.int32)] * (8 - len(known)))
    low = mask(iota((LANES, rows), 0) == (near & (LANES - 1))).astype(BF16)
    looked = dot(jnp.concatenate(known, axis=0).astype(BF16), low)
    kept = jnp.sum(jnp.where(iota(looked.shape, 0) == (near >> 7), looked, 0.0), axis=0, keepdims=True)
    named = jnp.where(iota((shards, rows), 0) == dest, kept, 0.0)
    named_b = named.astype(BF16)
    blk = LANES
    upper = mask((iota((blk, 2 * blk), 0) < iota((blk, 2 * blk), 1)) | (iota((blk, 2 * blk), 1) >= blk)).astype(BF16)
    before = jnp.zeros((shards, blk), F32)
    ranks = []
    for b in range(rows // blk):
        cut = slice(b * blk, (b + 1) * blk)
        both = dot(named_b[:, cut], upper)
        ranks.append(jnp.sum((both[:, :blk] + before) * named[:, cut], axis=0, keepdims=True))
        before = before + both[:, blk:]
    rank = jnp.concatenate(ranks, axis=1).astype(jnp.int32)
    counts = dot(jnp.ones((8, rows), BF16), named_b, NT)[:1]
    core, y = (dest >> log2(subs)) & 1, dest & (subs - 1)
    away = core ^ ((me[0] >> log2(subs)) & 1)
    chip = ((dest - core * subs - y) >> 1) + y
    slot = jnp.where(kept > 0.5, CAP * (away * chips + chip) + rank, -1)
    second = jnp.where(kept > 0.5, 2 * chip + 1, -1)
    at = 3 * iota((2 * shards, rows), 0)

    def place(j):
        picked = dot(mask(at == slot - j).astype(BF16), emb[...]).astype(BF16)
        for k in range(CORES):
            piece = picked[2 * chips * k : 2 * chips * (k + 1)].reshape(chips, 2, width)
            out[:, :, (HALF * k + j) * width : (HALF * k + j + 1) * width] = piece

    def class_scale(c):
        wide = table[c : min(c + CHUNK, classes), :].astype(F32)
        return lax.rsqrt(jnp.sum(wide * wide, axis=1, keepdims=True) + 1e-06)

    for move in moves[3:4]:
        move.wait()
    place(0)
    place(1)
    squares = []
    for b in range(rows // blk):
        part = emb[b * blk : (b + 1) * blk, :]
        gram = dot(part, part, NT)
        diag = iota((blk, blk), 0) == iota((blk, blk), 1)
        squares.append(jnp.sum(jnp.where(diag, gram, 0.0), axis=0, keepdims=True))
    inverse_row = lax.rsqrt(jnp.concatenate(squares, axis=1) + 1e-06)
    for move in moves[4:]:
        move.wait()
    scale = [class_scale(c) for c in range(0, classes, 1024)]
    given, others = [], []
    for r in range(0, rows, 256):
        cut = slice(r, r + 256)
        pair = jnp.zeros((1, 256), F32), jnp.full((1, 256), -jnp.inf, F32)
        for c in range(0, classes, 1024):
            size = min(1024, classes - c)
            scaled = dot(table[c : c + size, :], emb[cut, :], NT) * scale[c // 1024]
            match = iota((size, 256), 0) == near[:, cut] - c
            mine = jnp.sum(jnp.where(match, scaled, 0.0), axis=0, keepdims=True)
            best = jnp.max(jnp.where(match, -1e30, scaled), axis=0, keepdims=True)
            pair = pair[0] + mine, jnp.maximum(pair[1], best)
        given.append(pair[0])
        others.append(pair[1])
    given, others = jnp.concatenate(given, axis=1), jnp.concatenate(others, axis=1)
    score = (20.0 * (given - others) * inverse_row).astype(BF16).astype(F32)
    lane = (rank + CAP * me[0] + LANES // CORES * away) & (LANES - 1)
    spread = jnp.where(iota((LANES, rows), 0) == lane, score, 0.0).astype(BF16)
    place(2)
    scores = dot(mask(iota((2 * chips, rows), 0) == second).astype(BF16), spread, NT)
    more = jnp.where((iota((2 * chips, LANES), 0) & 1) == 0, counts, scores).astype(BF16)
    out[:, :, CAP * width :] = more.reshape(chips, 2, LANES)


def unpack_half(src, side, buf, rows_hbm, sems, between=None):
    owners, _, deep, width = rows_hbm.shape
    chips = owners * deep // CAP
    steps = sems.shape[0]
    m, q, part = CAP * chips // steps, 2 * chips // steps, owners // steps
    third = (iota((m, m), 0) * 21846) >> 16
    pick = mask(third + q * (iota((m, m), 0) - HALF * third) == iota((m, m), 1)).astype(BF16)
    moves = []
    for b in range(steps):
        if between and b == steps - 1:
            between()
        block = src(b * (q // 2), (b + 1) * (q // 2)).reshape(q, HALF * width)
        block = jnp.concatenate([block[:, j * width : (j + 1) * width] for j in range(HALF)], axis=0)
        cut = slice(b * part, (b + 1) * part)
        buf[cut] = dot(pick, block).astype(BF16).reshape(part, deep, width)
        move = pltpu.make_async_copy(buf.at[cut], rows_hbm.at[cut, side], sems.at[b])
        move.start()
        moves.append(move)
    return moves


def part_kernel(got, out):
    chips, _, chunk = out.shape
    for at in range(0, chunk, LANES):
        skip = got.shape[2] - chunk + at
        out[:, :, at : at + LANES] = got[:, :, skip : skip + LANES].reshape(2 * chips, LANES).reshape(chips, 2, LANES)


def own_kernel(me, got, rows_hbm, buf, sems):
    subs, width = rows_hbm.shape[2] // CAP, rows_hbm.shape[3]
    core = (me[0] >> log2(subs)) & 1
    for move in unpack_half(lambda a, b: got[a:b, :, : HALF * width], core, buf, rows_hbm, sems):
        move.wait()


def passed_kernel(
    me, got, passed, own_rows, rows_hbm, score_hbm, position_hbm, totals_hbm, buf, score_v, position_v, totals_v, extra, sems, late
):
    del own_rows
    subs, width = rows_hbm.shape[2] // CAP, rows_hbm.shape[3]
    chips = passed.shape[0]
    shards = CORES * chips
    core = (me[0] >> log2(subs)) & 1
    results = [(score_v, score_hbm), (position_v, position_hbm), (totals_v, totals_hbm)]
    small = [pltpu.make_async_copy(a, b, late.at[i]) for i, (a, b) in enumerate(results)]

    def between():
        extra[: 2 * chips] = got[:, :, CAP * width :].reshape(2 * chips, LANES).astype(F32)
        extra[2 * chips :] = passed[:, :, HALF * width :].reshape(2 * chips, LANES).astype(F32)
        counts, scores = extra[pl.ds(0, shards, stride=2), :], extra[pl.ds(1, shards, stride=2), :]
        scores = jnp.concatenate([scores[:chips], pltpu.roll(scores[chips:], LANES // CORES, 1)], axis=0)
        totals_v[...] = jnp.sum(counts, axis=0, keepdims=True).astype(jnp.int32)
        lane = iota((shards, LANES), 1) == me[0]
        own = jnp.sum(jnp.where(lane, counts, 0.0), axis=1, keepdims=True)
        i = iota((shards, LANES), 0)
        x, y = (i & (chips - 1)) >> log2(subs), i & (subs - 1)
        s = (CORES * x + jnp.where(i < chips, core, 1 - core)) * subs + y
        for a in range(CAP * shards // LANES):
            at = a * LANES + iota((1, LANES), 1)
            src = sixth(at)
            j = at - CAP * src
            here = s == src
            score = jnp.sum(jnp.where(here, scores, 0.0), axis=0, keepdims=True)
            held = jnp.sum(jnp.where(here, own, 0.0), axis=0, keepdims=True).astype(jnp.int32)
            ahead = jnp.sum(jnp.where(s < src, own, 0.0), axis=0, keepdims=True).astype(jnp.int32)
            score_v[a : a + 1, :] = score.astype(BF16)
            position_v[a : a + 1, :] = jnp.where(j < held, ahead + j, -1)
        for move in small:
            move.start()

    moves = unpack_half(lambda a, b: passed[a:b, :, : HALF * width], 1 - core, buf, rows_hbm, sems, between)
    for move in moves + small:
        move.wait()


def on_device(embeddings, class_table, nearest, keep_class, destination):
    shards, chips, owners, subs = (lax.axis_size(a) for a in (GROUP, CHIPS, "x", "sub"))
    rows, width = embeddings.shape
    classes = class_table.shape[0]
    chunk = CAP * width + LANES
    me = lax.axis_index(GROUP).reshape(1)
    vmem = pl.BlockSpec(memory_space=pltpu.VMEM)
    smem = pl.BlockSpec(memory_space=pltpu.SMEM)
    hbm = pl.BlockSpec(memory_space=pl.ANY)
    sent = pl.pallas_call(
        functools.partial(pack_kernel, subs),
        in_specs=[smem, hbm, hbm, hbm, hbm, hbm],
        out_specs=vmem,
        out_shape=pltpu.VMEM((chips, 2, chunk), BF16),
        scratch_shapes=[
            pltpu.VMEM((1, rows), jnp.int32),
            pltpu.VMEM((1, classes), jnp.int32),
            pltpu.VMEM((1, rows), jnp.int32),
            pltpu.VMEM((rows, width), BF16),
            pltpu.VMEM((classes, width), BF16),
            pltpu.SemaphoreType.DMA((4 + pl.cdiv(classes, CHUNK),)),
        ],
        name="pack",
    )(me, nearest.reshape(1, rows), keep_class.reshape(1, classes), destination.reshape(1, rows), embeddings, class_table)
    got = lax.all_to_all(sent, CHIPS, 0, 0, tiled=True)
    got = pltpu.with_memory_space_constraint(got, pltpu.VMEM)
    passed = pl.pallas_call(
        part_kernel,
        in_specs=[vmem],
        out_specs=vmem,
        out_shape=pltpu.VMEM((chips, 2, HALF * width + LANES), BF16),
        name="part",
    )(got)
    passed = lax.ppermute(passed, "core", [(0, 1), (1, 0)])
    slots = shards * CAP
    tall = slots // LANES
    rows_shape = jax.ShapeDtypeStruct((owners, CORES, CAP * subs, width), BF16)
    buf = pltpu.VMEM((owners, CAP * subs, width), BF16)
    own_rows = pl.pallas_call(
        own_kernel,
        in_specs=[smem, vmem],
        out_specs=hbm,
        out_shape=rows_shape,
        scratch_shapes=[buf, pltpu.SemaphoreType.DMA((2,))],
        name="own",
    )(me, got)
    received, score, position, totals = pl.pallas_call(
        passed_kernel,
        in_specs=[smem, vmem, vmem, hbm],
        out_specs=[hbm, hbm, hbm, hbm],
        out_shape=[
            rows_shape,
            jax.ShapeDtypeStruct((tall, LANES), BF16),
            jax.ShapeDtypeStruct((tall, LANES), jnp.int32),
            jax.ShapeDtypeStruct((1, shards), jnp.int32),
        ],
        scratch_shapes=[
            buf,
            pltpu.VMEM((tall, LANES), BF16),
            pltpu.VMEM((tall, LANES), jnp.int32),
            pltpu.VMEM((1, shards), jnp.int32),
            pltpu.VMEM((2 * shards, LANES), F32),
            pltpu.SemaphoreType.DMA((2,)),
            pltpu.SemaphoreType.DMA((3,)),
        ],
        input_output_aliases={3: 0},
        name="passed",
    )(me, got, pltpu.with_memory_space_constraint(passed, pltpu.VMEM), own_rows)
    return received.reshape(slots, width), score.reshape(slots), position.reshape(slots), totals.reshape(shards)


def solution(mesh):
    groups, owners, subs = (mesh.shape[a] for a in ("groups", "owners", "sub"))
    split = Mesh(mesh.devices.reshape(groups, owners // CORES, CORES, subs), ALL)
    return jax.shard_map(
        on_device,
        mesh=split,
        in_specs=(P(ALL, None), P(), P(ALL), P(), P(ALL, None)),
        out_specs=(P(ALL, None), P(ALL), P(ALL), P("groups")),
        check_vma=False,
    )
```
